8 devices in a mesh: data: 1 (over z), expert: 8 (over y, x, core).
Axes of the slice: x: 2, y: 2, z: 1, core: 2. Of those that a mesh axis runs over, the one named last changes fastest.
Arguments:
- x: bfloat16 [1024, 2048], P(('data', 'expert'))
- idx: int32 [1024, 8], P(('data', 'expert'))
- g: float32 [1024, 8], P(('data', 'expert'))
- hot_tok: int32 [512], P(('data', 'expert'))
- W1: bfloat16 [64, 2048, 1024], P('expert')
- W3: bfloat16 [64, 2048, 1024], P('expert')
- W2: bfloat16 [64, 1024, 2048], P('expert')
Outputs:
- output: bfloat16 [1024, 2048], P(('data', 'expert'))
All inputs are finite; a program needn't handle non-finite values.
Results may differ from the reference program's by a relative error of at most 0.001.
Values are sent between devices in bfloat16 or wider.
A program may use at most 1 GiB of HBM per device.

```python
import jax
import jax.numpy as jnp
from jax import lax

EXPERTS = 64
TOP = 8
D = 2048
FF = 1024
TOKENS = 128
HOT_DIV = 2
GROUP = 8

HOT_CAP = TOKENS // HOT_DIV
COLD_CAP = 2 * ((TOKENS * TOP - HOT_CAP + EXPERTS - 2) // (EXPERTS - 1))


def _weights(key, e, fan_in, fan_out):
    keys = jax.random.split(key, e)
    return lax.map(lambda k: (jax.random.normal(k, (fan_in, fan_out), jnp.float32) * fan_in ** -0.5).astype(jnp.bfloat16), keys)


def _chip_ids(key):
    k1, k2, k3 = jax.random.split(key, 3)
    t = jnp.arange(TOKENS)[:, None]
    j = jnp.arange(TOP)[None, :]
    hot = (t < HOT_CAP) & (j == 0)
    c = jnp.where(t < HOT_CAP, t * (TOP - 1) + j - 1, HOT_CAP * (TOP - 1) + (t - HOT_CAP) * TOP + j)
    seq = jnp.concatenate([jnp.arange(EXPERTS - 1), jnp.arange((EXPERTS - 1) // 2)])
    m = EXPERTS - 1 + (EXPERTS - 1) // 2
    off = jax.random.randint(k1, (), 0, m)
    perm = jax.random.permutation(k2, EXPERTS - 1)
    ids = jnp.flip(jnp.where(hot, 0, 1 + perm[seq[(c + off) % m]]), axis=1)
    shift = jax.random.randint(k3, (), 0, TOKENS)
    ids = jnp.roll(ids, shift, axis=0)
    hot_tok = jnp.sort((jnp.arange(HOT_CAP) + shift) % TOKENS)
    return ids.astype(jnp.int32), hot_tok.astype(jnp.int32)


def setup_inputs(seed: int = 0, part: int = 0) -> dict:
    kdata, kw = jax.random.split(jax.random.PRNGKey(seed))
    kx, kr, kg = jax.random.split(jax.random.fold_in(kdata, part), 3)
    k1, k3, k2 = jax.random.split(kw, 3)
    x = jax.random.normal(kx, (GROUP * TOKENS, D), jnp.float32).astype(jnp.bfloat16)
    ids, hot = jax.vmap(_chip_ids)(jax.random.split(jax.random.fold_in(kr, 7), GROUP))
    idx = ids.reshape(GROUP * TOKENS, TOP)
    u = jax.random.uniform(kg, (GROUP * TOKENS, TOP), jnp.float32)
    g = jnp.where(idx == 0, 0.6 + 0.4 * u, 0.2 + 0.5 * u)
    return {
        'x': x,
        'idx': idx,
        'g': g,
        'hot_tok': hot.reshape(GROUP * HOT_CAP),
        'W1': _weights(k1, EXPERTS, D, FF),
        'W3': _weights(k3, EXPERTS, D, FF),
        'W2': _weights(k2, EXPERTS, FF, D),
    }


def _expert(xr, w1, w3, w2):
    a = jnp.dot(xr, w1, preferred_element_type=jnp.float32)
    b = jnp.dot(xr, w3, preferred_element_type=jnp.float32)
    u = (jax.nn.silu(a) * b).astype(jnp.bfloat16)
    return jnp.dot(u, w2, preferred_element_type=jnp.float32).astype(jnp.bfloat16)


def reference(x, idx, g, hot_tok, W1, W3, W2):
    gate = jnp.where(idx == 0, g, 0.0).sum(axis=1)
    rows = (jnp.arange(GROUP)[:, None] * TOKENS + hot_tok.reshape(GROUP, HOT_CAP)).reshape(-1)
    hh = _expert(x[rows], W1[0], W3[0], W2[0]).astype(jnp.float32)
    y = jnp.zeros((GROUP * TOKENS, D), jnp.float32).at[rows].add(gate[rows][:, None] * hh)
    flat = idx.reshape(-1)
    order = jnp.argsort(flat, stable=True)
    counts = jnp.bincount(flat, length=EXPERTS)
    starts = jnp.cumsum(counts) - counts
    cap = GROUP * COLD_CAP
    order = jnp.concatenate([order, jnp.zeros((cap,), order.dtype)])
    gflat = g.reshape(-1)

    def step(y, ew):
        e, w1, w3, w2 = ew
        r = lax.dynamic_slice(order, (starts[e],), (cap,))
        valid = jnp.arange(cap) < counts[e]
        he = _expert(x[r // TOP], w1, w3, w2).astype(jnp.float32)
        return y.at[r // TOP].add(jnp.where(valid[:, None], gflat[r][:, None] * he, 0.0)), None

    y, _ = lax.scan(step, y, (jnp.arange(1, EXPERTS), W1[1:], W3[1:], W2[1:]))
    return y.astype(jnp.bfloat16)
```

```python
import functools

import jax
import jax.numpy as jnp
from jax import lax
from jax.experimental import pallas as pl
from jax.experimental.pallas import tpu as pltpu
from jax.sharding import PartitionSpec as P

BF = jnp.bfloat16
F32 = jnp.float32
BF_MAX = 3.3895313892515355e38
T = 128
D = 2048
FF = 1024
EL = 8
N = 8
CAP = 32
RB = EL * CAP + CAP
KC = 4
KW = D // KC
NC = 8
NW = D // NC
NS = 6
FWD_AT = 5


def _dot(a, b):
    return jnp.dot(a, b, preferred_element_type=F32)


def _kernel(tab_ref, x_ref, w1_ref, w3_ref, w2_ref, y_ref,
            tabs, xall, onehot, gates, xs, acc, u, ring1, ring2, hbuf, ybuf, r1, r2, r3,
            tab_s, tab_r, ag_s, ag_r, w1_sem, w2_sem, d_s, d_r, s1_s, s1_r, s2_s, s2_r):
    me = lax.axis_index('expert')
    core, xb, yb = me % 2, (me // 2) % 2, me // 4

    def peer(mask):
        return {'expert': me + (mask & 1) * (1 - 2 * core) + ((mask >> 1) & 1) * (2 - 4 * xb) + (mask >> 2) * (4 - 8 * yb)}

    def remote(src, dst, ssem, rsem, mask):
        return pltpu.make_async_remote_copy(src_ref=src, dst_ref=dst, send_sem=ssem, recv_sem=rsem,
                                            device_id=peer(mask), device_id_type=pl.DeviceIdType.MESH)

    def up_copies(kc, e, slot):
        rows = pl.ds(kc * KW, KW)
        return (pltpu.make_async_copy(w1_ref.at[e, rows, :], ring1.at[slot, 0], w1_sem.at[slot, 0]),
                pltpu.make_async_copy(w3_ref.at[e, rows, :], ring1.at[slot, 1], w1_sem.at[slot, 1]))

    def down_copy(nc, e):
        return pltpu.make_async_copy(w2_ref.at[e, :, pl.ds(nc * NW, NW)], ring2.at[e], w2_sem.at[e])

    for i in range(NS):
        for c in up_copies(i // EL, i % EL, i):
            c.start()

    barrier = pltpu.get_barrier_semaphore()
    for mask in range(1, N):
        pl.semaphore_signal(barrier, inc=1, device_id=peer(mask), device_id_type=pl.DeviceIdType.MESH)
    pl.semaphore_wait(barrier, N - 1)

    def tab_copy(mask):
        return remote(tab_ref, tabs.at[mask], tab_s.at[mask], tab_r.at[mask], mask)

    def ag_copy(c, mask):
        return remote(x_ref.at[:, pl.ds(c * KW, KW)], xall.at[c, mask], ag_s.at[c, mask], ag_r.at[c, mask], mask)

    def fwd_copy(c, mask):
        return remote(xall.at[c, mask], xall.at[c, mask + 1], ag_s.at[c, mask + 1], ag_r.at[c, mask + 1], 1)

    for mask in range(1, N):
        tab_copy(mask).start()
    for c in range(KC):
        for mask in (6, 2, 4, 1):
            ag_copy(c, mask).start()
    tabs[0] = tab_ref[...]
    for c in range(KC):
        xall[c, 0] = x_ref[:, c * KW:(c + 1) * KW]
    for mask in range(1, N):
        tab_copy(mask).wait_recv()

    base = (me * EL).astype(F32)
    ids = lax.broadcasted_iota(jnp.int32, (EL, T), 0).astype(F32) + base
    sels, gs = [], []
    for r in range(N):
        sel = jnp.zeros((EL, T), F32)
        gate = jnp.zeros((EL, T), F32)
        tab = tabs[r]
        for j in range(8):
            hit = jnp.broadcast_to(tab[j:j + 1], (EL, T)) == ids
            sel = jnp.where(hit, 1.0, sel)
            gate = jnp.where(hit, jnp.broadcast_to(tab[8 + j:9 + j], (EL, T)), gate)
        sels.append(sel)
        gs.append(gate)
    sel_all = jnp.concatenate(sels, axis=0)
    upper = (lax.broadcasted_iota(jnp.int32, (T, T), 0) < lax.broadcasted_iota(jnp.int32, (T, T), 1))
    upper = jnp.where(upper, 1.0, 0.0).astype(BF)
    rank_all = jnp.where(sel_all > 0.5, _dot(sel_all.astype(BF), upper), -1.0)

    col = lax.broadcasted_iota(jnp.int32, (32, RB), 1)
    row = lax.broadcasted_iota(jnp.int32, (32, RB), 0)
    owner = jnp.where(col < EL * CAP, col // CAP, 0)
    pick = [jnp.where(row == q * EL + owner, 1.0, 0.0).astype(BF) for q in range(4)]
    colt = lax.broadcasted_iota(jnp.int32, (T, RB), 1)
    slot_of = jnp.where(colt < EL * CAP, colt % CAP, colt - EL * CAP + CAP).astype(F32)
    sub = lax.broadcasted_iota(jnp.int32, (CAP, T), 0).astype(F32)
    for r in range(N):
        rk = rank_all[r * EL:(r + 1) * EL]
        for b in range(EL + 1):
            want = sub if b < EL else sub + CAP
            src = b % EL
            hit = jnp.broadcast_to(rk[src:src + 1], (CAP, T)) == want
            onehot[r, b * CAP:(b + 1) * CAP, :] = jnp.where(hit, 1.0, 0.0).astype(BF)
        g = gs[r]
        g1 = jnp.minimum(g, BF_MAX).astype(BF).astype(F32)
        rem = g - g1
        g2 = rem.astype(BF).astype(F32)
        g3 = rem - g2
        v = jnp.concatenate([rk, g1, g2, g3], axis=0)
        vt = v.T.astype(BF)
        hit = _dot(vt, pick[0]) == slot_of
        for q in range(3):
            gates[r, q * T:(q + 1) * T, :] = jnp.where(hit, _dot(vt, pick[q + 1]), 0.0).astype(BF)

    def forward(c):
        for mask in (2, 4, 6):
            ag_copy(c, mask).wait_recv()
            fwd_copy(c, mask).start()

    forward(0)
    for kc in range(KC):
        ag_copy(kc, 1).wait_recv()
        for mask in (2, 4, 6):
            fwd_copy(kc, mask).wait_recv()

        def dispatch(r, _, kc=kc):
            rows = _dot(onehot[r], xall[kc, r]).astype(BF)
            at = pl.ds(pl.multiple_of(r * CAP, CAP), CAP)
            for b in range(EL + 1):
                xs[b, at, :] = rows[b * CAP:(b + 1) * CAP]
            return 0
        lax.fori_loop(0, N, dispatch, 0)

        def block(b, slot, kc=kc):
            xb_ = xs[b]
            for n in range(FF // 256):
                cols = slice(n * 256, (n + 1) * 256)
                a = _dot(xb_, ring1[slot, 0, :, cols])
                bb = _dot(xb_, ring1[slot, 1, :, cols])
                if kc > 0:
                    a = a + acc[0, b, :, cols]
                    bb = bb + acc[1, b, :, cols]
                if kc < KC - 1:
                    acc[0, b, :, cols] = a
                    acc[1, b, :, cols] = bb
                else:
                    u[b, :, cols] = (jax.nn.silu(a) * bb).astype(BF)

        def step(e, _, kc=kc):
            i = kc * EL + e
            slot = i % NS
            for c in up_copies(kc, e, slot):
                c.wait()
            block(e, slot)

            @pl.when(e == 0)
            def _():
                block(EL, slot)

            nxt = i + NS

            @pl.when(nxt < KC * EL)
            def _():
                for c in up_copies(nxt // EL, nxt % EL, slot):
                    c.start()

            if kc + 1 < KC:
                @pl.when(e == FWD_AT)
                def _():
                    forward(kc + 1)
            if kc == KC - 2:
                down_copy(0, e).start()
            return 0
        lax.fori_loop(0, EL, step, 0)

    def d_copy(nc):
        return remote(ybuf.at[nc % 2, 1], r1.at[nc], d_s.at[nc], d_r.at[nc], 1)

    def s1_copies(nc):
        return (remote(r1.at[nc, :, 1, pl.ds(0, 64), :], r2.at[nc, 0], s1_s.at[nc, 0], s1_r.at[nc, 0], 2),
                remote(r1.at[nc, 1, :, pl.ds(64, 64), :], r2.at[nc, 1], s1_s.at[nc, 1], s1_r.at[nc, 1], 4))

    def s2_copies(nc):
        return (remote(r2.at[nc, 0, 1], r3.at[nc, 0], s2_s.at[nc, 0], s2_r.at[nc, 0], 4),
                remote(r2.at[nc, 1, 1], r3.at[nc, 1], s2_s.at[nc, 1], s2_r.at[nc, 1], 2))

    def stage1(nc):
        d_copy(nc).wait_recv()
        for q in range(4):
            r1[nc, q // 2, q % 2] = r1[nc, q // 2, q % 2] + ybuf[nc % 2, 0, q // 2, q % 2]
        for c in s1_copies(nc):
            c.start()

    def stage2(nc):
        ca, cb = s1_copies(nc)
        sa, sb = s2_copies(nc)
        ca.wait_recv()
        r2[nc, 0, 1] = r2[nc, 0, 1] + r1[nc, 1, 0, 0:64]
        sa.start()
        cb.wait_recv()
        r2[nc, 1, 1] = r2[nc, 1, 1] + r1[nc, 0, 1, 64:128]
        sb.start()

    def final(nc):
        for h, c in enumerate(s2_copies(nc)):
            c.wait_recv()
            rows = slice(h * 64, h * 64 + 64)
            val = r1[nc, 0, 0, rows] + r2[nc, h, 0] + r3[nc, h]
            y_ref[rows, pl.ds(pl.multiple_of(nc * NW, NW), NW)] = val.astype(BF)

    def out_step(nc, _):
        def down(e, _):
            down_copy(nc, e).wait()

            def put(b):
                h = _dot(u[b], ring2[e]).astype(BF)
                at = pl.ds(pl.multiple_of(b * CAP, CAP), CAP)
                for r in range(N):
                    hbuf[r, at, :] = h[r * CAP:(r + 1) * CAP]
            put(e)

            @pl.when(e == 0)
            def _():
                put(EL)

            @pl.when(nc + 1 < NC)
            def _():
                down_copy(nc + 1, e).start()
            return 0
        lax.fori_loop(0, EL, down, 0)

        @pl.when(nc >= 2)
        def _():
            d_copy(nc - 2).wait_send()

        def combine(r, _):
            part = _dot(gates[r], hbuf[r])
            ybuf[nc % 2, r % 2, r // 4, (r // 2) % 2] = part[0:T] + part[T:2 * T] + part[2 * T:3 * T]
            return 0
        lax.fori_loop(0, N, combine, 0)
        d_copy(nc).start()

        @pl.when(nc >= 1)
        def _():
            stage1(nc - 1)

        @pl.when(nc >= 2)
        def _():
            stage2(nc - 2)

        @pl.when(nc >= 4)
        def _():
            final(nc - 4)
        return 0
    lax.fori_loop(0, NC, out_step, 0)
    stage1(NC - 1)
    stage2(NC - 2)
    final(NC - 4)
    final(NC - 3)
    stage2(NC - 1)
    final(NC - 2)
    final(NC - 1)

    for mask in range(1, N):
        tab_copy(mask).wait_send()
    for c in range(KC):
        for mask in (1, 2, 4, 6):
            ag_copy(c, mask).wait_send()
        for mask in (2, 4, 6):
            fwd_copy(c, mask).wait_send()
    for nc in range(NC):
        if nc >= NC - 2:
            d_copy(nc).wait_send()
        for c in s1_copies(nc) + s2_copies(nc):
            c.wait_send()


def _moe(tab, x, w1, w3, w2):
    dma = pltpu.SemaphoreType.DMA
    vm, hbm = pl.BlockSpec(memory_space=pltpu.VMEM), pl.BlockSpec(memory_space=pl.ANY)
    return pl.pallas_call(
        _kernel,
        out_shape=jax.ShapeDtypeStruct((T, D), BF),
        in_specs=[vm, vm, hbm, hbm, hbm],
        out_specs=vm,
        scratch_shapes=[
            pltpu.VMEM((N, 16, T), F32),
            pltpu.VMEM((KC, N, T, KW), BF),
            pltpu.VMEM((N, RB, T), BF),
            pltpu.VMEM((N, 3 * T, RB), BF),
            pltpu.VMEM((EL + 1, N * CAP, KW), BF),
            pltpu.VMEM((2, EL + 1, N * CAP, FF), F32),
            pltpu.VMEM((EL + 1, N * CAP, FF), BF),
            pltpu.VMEM((NS, 2, KW, FF), BF),
            pltpu.VMEM((EL, FF, NW), BF),
            pltpu.VMEM((N, RB, NW), BF),
            pltpu.VMEM((2, 2, 2, 2, T, NW), F32),
            pltpu.VMEM((NC, 2, 2, T, NW), F32),
            pltpu.VMEM((NC, 2, 2, 64, NW), F32),
            pltpu.VMEM((NC, 2, 64, NW), F32),
            dma((N,)), dma((N,)),
            dma((KC, N)), dma((KC, N)),
            dma((NS, 2)), dma((EL,)),
            dma((NC,)), dma((NC,)),
            dma((NC, 2)), dma((NC, 2)),
            dma((NC, 2)), dma((NC, 2)),
        ],
        compiler_params=pltpu.CompilerParams(collective_id=0, has_side_effects=True, vmem_limit_bytes=67043328),
        name='moe',
    )(tab, x, w1, w3, w2)


def solution(mesh):
    def local(x, idx, g, hot_tok, w1, w3, w2):
        tab = jnp.concatenate([idx.T.astype(F32), g.T], axis=0)
        return _moe(tab, x, w1, w3, w2)

    rows = P(('data', 'expert'))
    wspec = P('expert')
    return jax.shard_map(local, mesh=mesh, in_specs=(rows, rows, rows, rows, wspec, wspec, wspec), out_specs=rows, check_vma=False)
```

```python
import functools

import jax
import jax.numpy as jnp
from jax import lax
from jax.experimental import pallas as pl
from jax.experimental.pallas import tpu as pltpu
from jax.sharding import PartitionSpec as P

BF = jnp.bfloat16
F32 = jnp.float32
BF_MAX = 3.3895313892515355e38
T = 128
D = 2048
FF = 1024
EL = 8
N = 8
CAP = 32
RB = EL * CAP + CAP
KC = 4
KW = D // KC
NC = 8
NW = D // NC
EP = 2
NP = EL // EP
NS = 3
FWD_AT = 2
CHIP = (0, 3, 1, 2)


def _dot(a, b):
    return jnp.dot(a, b, preferred_element_type=F32)


def _kernel(tab_ref, x_ref, w1_ref, w3_ref, w2_ref, y_ref,
            tabs, xall, onehot, gates, xs, acc, u, ring1, ring2, hbuf, r1, r2, r3,
            tab_s, tab_r, ag_s, ag_r, w1_sem, w2_sem, d_s, d_r, s1_s, s1_r, s2_s, s2_r):
    me = lax.axis_index('expert')
    core, xb, yb = me % 2, (me // 2) % 2, me // 4

    def peer(mask):
        return {'expert': me + (mask & 1) * (1 - 2 * core) + ((mask >> 1) & 1) * (2 - 4 * xb) + (mask >> 2) * (4 - 8 * yb)}

    def remote(src, dst, ssem, rsem, mask):
        return pltpu.make_async_remote_copy(src_ref=src, dst_ref=dst, send_sem=ssem, recv_sem=rsem,
                                            device_id=peer(mask), device_id_type=pl.DeviceIdType.MESH)

    def up_copies(kc, p, slot):
        rows = pl.ds(kc * KW, KW)
        es = pl.ds(p * EP, EP)
        return (pltpu.make_async_copy(w1_ref.at[es, rows, :], ring1.at[slot, 0], w1_sem.at[slot, 0]),
                pltpu.make_async_copy(w3_ref.at[es, rows, :], ring1.at[slot, 1], w1_sem.at[slot, 1]))

    def down_copy(nc):
        return pltpu.make_async_copy(w2_ref.at[:, :, pl.ds(nc * NW, NW)], ring2.at[nc % 2], w2_sem.at[nc % 2])

    for i in range(NS):
        for c in up_copies(i // NP, i % NP, i):
            c.start()

    barrier = pltpu.get_barrier_semaphore()
    for mask in range(1, N):
        pl.semaphore_signal(barrier, inc=1, device_id=peer(mask), device_id_type=pl.DeviceIdType.MESH)
    pl.semaphore_wait(barrier, N - 1)

    def tab_copy(mask):
        return remote(tab_ref, tabs.at[mask], tab_s.at[mask], tab_r.at[mask], mask)

    def ag_copy(c, mask):
        return remote(x_ref.at[:, pl.ds(c * KW, KW)], xall.at[c, mask], ag_s.at[c, mask], ag_r.at[c, mask], mask)

    def fwd_copy(c, mask):
        return remote(xall.at[c, mask], xall.at[c, mask + 1], ag_s.at[c, mask + 1], ag_r.at[c, mask + 1], 1)

    for mask in range(1, N):
        tab_copy(mask).start()
    for c in range(KC):
        for mask in (6, 2, 4, 1):
            ag_copy(c, mask).start()
    tabs[0] = tab_ref[...]
    for c in range(KC):
        xall[c, 0] = x_ref[:, c * KW:(c + 1) * KW]
    for mask in range(1, N):
        tab_copy(mask).wait_recv()

    base = (me * EL).astype(F32)
    ids = lax.broadcasted_iota(jnp.int32, (EL, T), 0).astype(F32) + base
    sels, gs = [], []
    for r in range(N):
        sel = jnp.zeros((EL, T), F32)
        gate = jnp.zeros((EL, T), F32)
        tab = tabs[r]
        for j in range(8):
            hit = jnp.broadcast_to(tab[j:j + 1], (EL, T)) == ids
            sel = jnp.where(hit, 1.0, sel)
            gate = jnp.where(hit, jnp.broadcast_to(tab[8 + j:9 + j], (EL, T)), gate)
        sels.append(sel)
        gs.append(gate)
    sel_all = jnp.concatenate(sels, axis=0)
    upper = (lax.broadcasted_iota(jnp.int32, (T, T), 0) < lax.broadcasted_iota(jnp.int32, (T, T), 1))
    upper = jnp.where(upper, 1.0, 0.0).astype(BF)
    rank_all = jnp.where(sel_all > 0.5, _dot(sel_all.astype(BF), upper), -1.0)

    col = lax.broadcasted_iota(jnp.int32, (32, RB), 1)
    row = lax.broadcasted_iota(jnp.int32, (32, RB), 0)
    owner = jnp.where(col < EL * CAP, col // CAP, 0)
    pick = [jnp.where(row == q * EL + owner, 1.0, 0.0).astype(BF) for q in range(4)]
    colt = lax.broadcasted_iota(jnp.int32, (T, RB), 1)
    slot_of = jnp.where(colt < EL * CAP, colt % CAP, colt - EL * CAP + CAP).astype(F32)
    sub = lax.broadcasted_iota(jnp.int32, (CAP, T), 0).astype(F32)
    for r in range(N):
        rk = rank_all[r * EL:(r + 1) * EL]
        for b in range(EL + 1):
            want = sub if b < EL else sub + CAP
            src = b % EL
            hit = jnp.broadcast_to(rk[src:src + 1], (CAP, T)) == want
            onehot[r, b * CAP:(b + 1) * CAP, :] = jnp.where(hit, 1.0, 0.0).astype(BF)
        g = gs[r]
        g1 = jnp.minimum(g, BF_MAX).astype(BF).astype(F32)
        rem = g - g1
        g2 = rem.astype(BF).astype(F32)
        g3 = rem - g2
        v = jnp.concatenate([rk, g1, g2, g3], axis=0)
        vt = v.T.astype(BF)
        hit = _dot(vt, pick[0]) == slot_of
        for q in range(3):
            gates[r, q * T:(q + 1) * T, :] = jnp.where(hit, _dot(vt, pick[q + 1]), 0.0).astype(BF)

    def forward(c):
        for mask in (2, 4, 6):
            ag_copy(c, mask).wait_recv()
            fwd_copy(c, mask).start()

    forward(0)
    for kc in range(KC):
        ag_copy(kc, 1).wait_recv()
        for mask in (2, 4, 6):
            fwd_copy(kc, mask).wait_recv()

        for r in range(N):
            rows = _dot(onehot[r], xall[kc, r]).astype(BF)
            for b in range(EL + 1):
                xs[b, r * CAP:(r + 1) * CAP, :] = rows[b * CAP:(b + 1) * CAP]

        def block(b, slot, q, kc=kc):
            xb_ = xs[b]
            for n in range(FF // 256):
                cols = slice(n * 256, (n + 1) * 256)
                a = _dot(xb_, ring1[slot, 0, q, :, cols])
                bb = _dot(xb_, ring1[slot, 1, q, :, cols])
                if kc > 0:
                    a = a + acc[0, b, :, cols]
                    bb = bb + acc[1, b, :, cols]
                if kc < KC - 1:
                    acc[0, b, :, cols] = a
                    acc[1, b, :, cols] = bb
                else:
                    u[b, :, cols] = (jax.nn.silu(a) * bb).astype(BF)

        def step(p, _, kc=kc):
            i = kc * NP + p
            slot = i % NS
            for c in up_copies(kc, p, slot):
                c.wait()
            for q in range(EP):
                block(p * EP + q, slot, q)

            @pl.when((p == 0) & (me == 0))
            def _():
                block(EL, slot, 0)

            nxt = i + NS

            @pl.when(nxt < KC * NP)
            def _():
                for c in up_copies(nxt // NP, nxt % NP, slot):
                    c.start()

            if kc + 1 < KC:
                @pl.when(p == FWD_AT)
                def _():
                    forward(kc + 1)
            if kc == KC - 1:
                @pl.when(p < 2)
                def _():
                    down_copy(p).start()
            return 0
        lax.fori_loop(0, NP, step, 0)

    def d_copy(nc):
        return remote(acc.at[nc % 2, pl.ds(4, 4), pl.ds(0, T), pl.ds(0, NW)], r1.at[nc], d_s.at[nc], d_r.at[nc], 1)

    def s1_copies(nc):
        return (remote(r1.at[nc, pl.ds(2, 2), pl.ds(0, 64), :], r2.at[nc, 0], s1_s.at[nc, 0], s1_r.at[nc, 0], 2),
                remote(r1.at[nc, pl.ds(1, 2), pl.ds(64, 64), :], r2.at[nc, 1], s1_s.at[nc, 1], s1_r.at[nc, 1], 4))

    def s2_copies(nc):
        return (remote(r2.at[nc, 0, 0], r3.at[nc, 0], s2_s.at[nc, 0], s2_r.at[nc, 0], 4),
                remote(r2.at[nc, 1, 1], r3.at[nc, 1], s2_s.at[nc, 1], s2_r.at[nc, 1], 2))

    def stage1(nc):
        d_copy(nc).wait_recv()
        for q in range(4):
            r1[nc, q] = r1[nc, q] + acc[nc % 2, q, 0:T, 0:NW]
        for c in s1_copies(nc):
            c.start()

    def stage2(nc):
        ca, cb = s1_copies(nc)
        sa, sb = s2_copies(nc)
        ca.wait_recv()
        r2[nc, 0, 0] = r2[nc, 0, 0] + r1[nc, 1, 0:64]
        sa.start()
        cb.wait_recv()
        r2[nc, 1, 1] = r2[nc, 1, 1] + r1[nc, 3, 64:128]
        sb.start()

    def final(nc):
        for h, c in enumerate(s2_copies(nc)):
            c.wait_recv()
            rows = slice(h * 64, h * 64 + 64)
            val = r1[nc, 0, rows] + r2[nc, h, 1 - h] + r3[nc, h]
            y_ref[rows, pl.ds(pl.multiple_of(nc * NW, NW), NW)] = val.astype(BF)

    def out_step(nc, _):
        down_copy(nc).wait()

        def put(b, e):
            h = _dot(u[b], ring2[nc % 2, e]).astype(BF)
            for r in range(N):
                hbuf[r, b * CAP:(b + 1) * CAP, :] = h[r * CAP:(r + 1) * CAP]
        for e in range(EL):
            put(e, e)

        @pl.when(me == 0)
        def _():
            put(EL, 0)

        @pl.when(nc + 2 < NC)
        def _():
            down_copy(nc + 2).start()

        @pl.when(nc >= 1)
        def _():
            stage1(nc - 1)

        @pl.when(nc >= 2)
        def _():
            d_copy(nc - 2).wait_send()

        def combine(rows):
            for r in range(N):
                part = _dot(gates[r, :, 0:rows], hbuf[r, 0:rows, :])
                acc[nc % 2, 4 * (r % 2) + CHIP[r // 2], 0:T, 0:NW] = part[0:T] + part[T:2 * T] + part[2 * T:3 * T]

        @pl.when(me == 0)
        def _():
            combine(RB)

        @pl.when(me != 0)
        def _():
            combine(EL * CAP)

        d_copy(nc).start()

        @pl.when(nc >= 3)
        def _():
            stage2(nc - 3)

        @pl.when(nc >= 5)
        def _():
            final(nc - 5)
        return 0
    lax.fori_loop(0, NC, out_step, 0)
    stage1(NC - 1)
    stage2(NC - 3)
    final(NC - 5)
    stage2(NC - 2)
    final(NC - 4)
    stage2(NC - 1)
    for nc in range(NC - 3, NC):
        final(nc)

    for mask in range(1, N):
        tab_copy(mask).wait_send()
    for c in range(KC):
        for mask in (1, 2, 4, 6):
            ag_copy(c, mask).wait_send()
        for mask in (2, 4, 6):
            fwd_copy(c, mask).wait_send()
    for nc in range(NC):
        if nc >= NC - 2:
            d_copy(nc).wait_send()
        for c in s1_copies(nc) + s2_copies(nc):
            c.wait_send()


def _moe(tab, x, w1, w3, w2):
    dma = pltpu.SemaphoreType.DMA
    vm, hbm = pl.BlockSpec(memory_space=pltpu.VMEM), pl.BlockSpec(memory_space=pl.ANY)
    return pl.pallas_call(
        _kernel,
        out_shape=jax.ShapeDtypeStruct((T, D), BF),
        in_specs=[vm, vm, hbm, hbm, hbm],
        out_specs=vm,
        scratch_shapes=[
            pltpu.VMEM((N, 16, T), F32),
            pltpu.VMEM((KC, N, T, KW), BF),
            pltpu.VMEM((N, RB, T), BF),
            pltpu.VMEM((N, 3 * T, RB), BF),
            pltpu.VMEM((EL + 1, N * CAP, KW), BF),
            pltpu.VMEM((2, EL + 1, N * CAP, FF), F32),
            pltpu.VMEM((EL + 1, N * CAP, FF), BF),
            pltpu.VMEM((NS, 2, EP, KW, FF), BF),
            pltpu.VMEM((2, EL, FF, NW), BF),
            pltpu.VMEM((N, RB, NW), BF),
            pltpu.VMEM((NC, 4, T, NW), F32),
            pltpu.VMEM((NC, 2, 2, 64, NW), F32),
            pltpu.VMEM((NC, 2, 64, NW), F32),
            dma((N,)), dma((N,)),
            dma((KC, N)), dma((KC, N)),
            dma((NS, 2)), dma((2,)),
            dma((NC,)), dma((NC,)),
            dma((NC, 2)), dma((NC, 2)),
            dma((NC, 2)), dma((NC, 2)),
        ],
        compiler_params=pltpu.CompilerParams(collective_id=0, has_side_effects=True, vmem_limit_bytes=67043328),
        name='moe',
    )(tab, x, w1, w3, w2)


def solution(mesh):
    def local(x, idx, g, hot_tok, w1, w3, w2):
        tab = jnp.concatenate([idx.T.astype(F32), g.T], axis=0)
        return _moe(tab, x, w1, w3, w2)

    rows = P(('data', 'expert'))
    wspec = P('expert')
    return jax.shard_map(local, mesh=mesh, in_specs=(rows, rows, rows, rows, wspec, wspec, wspec), out_specs=rows, check_vma=False)
```

```python
import functools

import jax
import jax.numpy as jnp
from jax import lax
from jax.experimental import pallas as pl
from jax.experimental.pallas import tpu as pltpu
from jax.sharding import PartitionSpec as P

BF = jnp.bfloat16
F32 = jnp.float32
BF_MAX = 3.3895313892515355e38
T = 128
D = 2048
FF = 1024
EL = 8
N = 8
CAP = 32
RB = EL * CAP + CAP
CHUNKS = ((0, 256), (256, 256), (512, 512), (1024, 512), (1536, 512))
KC = len(CHUNKS)
KW = 512
NC = 8
NW = D // NC
EP = 2
NP = EL // EP
NS = 3
FWD_AT = 2
CHIP = (0, 3, 1, 2)


def _dot(a, b):
    return jnp.dot(a, b, preferred_element_type=F32)


def _kernel(idx_ref, g_ref, x_ref, w1_ref, w3_ref, w2_ref, y_ref,
            idxs, gs, xsmall, xbig, onehot, gates, xs, acc, u, ring1, ring2, hbuf, r1, r2, r3,
            tab_s, tab_r, gt_s, gt_r, ag_s, ag_r, w1_sem, w2_sem, d_s, d_r, s1_s, s1_r, s2_s, s2_r):
    me = lax.axis_index('expert')
    core, xb, yb = me % 2, (me // 2) % 2, me // 4

    def peer(mask):
        return {'expert': me + (mask & 1) * (1 - 2 * core) + ((mask >> 1) & 1) * (2 - 4 * xb) + (mask >> 2) * (4 - 8 * yb)}

    def remote(src, dst, ssem, rsem, mask):
        return pltpu.make_async_remote_copy(src_ref=src, dst_ref=dst, send_sem=ssem, recv_sem=rsem,
                                            device_id=peer(mask), device_id_type=pl.DeviceIdType.MESH)

    def up_copies(kc, p, slot):
        rows = pl.ds(*CHUNKS[kc])
        to = pl.ds(0, CHUNKS[kc][1])
        es = pl.ds(p * EP, EP)
        return (pltpu.make_async_copy(w1_ref.at[es, rows, :], ring1.at[slot, 0, :, to, :], w1_sem.at[slot, 0]),
                pltpu.make_async_copy(w3_ref.at[es, rows, :], ring1.at[slot, 1, :, to, :], w1_sem.at[slot, 1]))

    def down_copy(nc):
        return pltpu.make_async_copy(w2_ref.at[:, :, pl.ds(nc * NW, NW)], ring2.at[nc % 2], w2_sem.at[nc % 2])

    for i in range(NS):
        for c in up_copies(0, i, i):
            c.start()

    barrier = pltpu.get_barrier_semaphore()
    for mask in range(1, N):
        pl.semaphore_signal(barrier, inc=1, device_id=peer(mask), device_id_type=pl.DeviceIdType.MESH)
    pl.semaphore_wait(barrier, N - 1)

    def table_copies(mask):
        return (remote(idx_ref, idxs.at[mask], tab_s.at[mask], tab_r.at[mask], mask),
                remote(g_ref, gs.at[mask], gt_s.at[mask], gt_r.at[mask], mask))

    def table_fwd(mask):
        return (remote(idxs.at[mask], idxs.at[mask + 1], tab_s.at[mask + 1], tab_r.at[mask + 1], 1),
                remote(gs.at[mask], gs.at[mask + 1], gt_s.at[mask + 1], gt_r.at[mask + 1], 1))

    def part(c, mask):
        return xsmall.at[c, mask] if c < 2 else xbig.at[c - 2, mask]

    def ag_copy(c, mask):
        return remote(x_ref.at[:, pl.ds(*CHUNKS[c])], part(c, mask), ag_s.at[c, mask], ag_r.at[c, mask], mask)

    def fwd_copy(c, mask):
        return remote(part(c, mask), part(c, mask + 1), ag_s.at[c, mask + 1], ag_r.at[c, mask + 1], 1)

    for mask in (6, 2, 4, 1):
        for c in table_copies(mask):
            c.start()
    for c in range(KC):
        for mask in (6, 2, 4, 1):
            ag_copy(c, mask).start()
    idxs[0] = idx_ref[...]
    gs[0] = g_ref[...]
    for c, (first, width) in enumerate(CHUNKS):
        part(c, 0)[...] = x_ref[:, first:first + width]
    for mask in (2, 4, 6):
        for c in table_copies(mask):
            c.wait_recv()
        for c in table_fwd(mask):
            c.start()
    for c in table_copies(1):
        c.wait_recv()
    for mask in (2, 4, 6):
        for c in table_fwd(mask):
            c.wait_recv()

    ids = lax.broadcasted_iota(jnp.int32, (EL, T), 0) + me * EL
    sels, weights = [], []
    for r in range(N):
        sel = jnp.zeros((EL, T), F32)
        gate = jnp.zeros((EL, T), F32)
        tab, gtab = idxs[r], gs[r]
        for j in range(8):
            hit = jnp.broadcast_to(tab[j:j + 1], (EL, T)) == ids
            sel = jnp.where(hit, 1.0, sel)
            gate = jnp.where(hit, jnp.broadcast_to(gtab[j:j + 1], (EL, T)), gate)
        sels.append(sel)
        weights.append(gate)
    sel_all = jnp.concatenate(sels, axis=0)
    upper = (lax.broadcasted_iota(jnp.int32, (T, T), 0) < lax.broadcasted_iota(jnp.int32, (T, T), 1))
    upper = jnp.where(upper, 1.0, 0.0).astype(BF)
    rank_all = jnp.where(sel_all > 0.5, _dot(sel_all.astype(BF), upper), -1.0)

    col = lax.broadcasted_iota(jnp.int32, (32, RB), 1)
    row = lax.broadcasted_iota(jnp.int32, (32, RB), 0)
    owner = jnp.where(col < EL * CAP, col // CAP, 0)
    pick = [jnp.where(row == q * EL + owner, 1.0, 0.0).astype(BF) for q in range(4)]
    colt = lax.broadcasted_iota(jnp.int32, (T, RB), 1)
    slot_of = jnp.where(colt < EL * CAP, colt % CAP, colt - EL * CAP + CAP).astype(F32)
    sub = lax.broadcasted_iota(jnp.int32, (CAP, T), 0).astype(F32)
    for r in range(N):
        rk = rank_all[r * EL:(r + 1) * EL]
        for b in range(EL + 1):
            want = sub if b < EL else sub + CAP
            src = b % EL
            hit = jnp.broadcast_to(rk[src:src + 1], (CAP, T)) == want
            onehot[r, b * CAP:(b + 1) * CAP, :] = jnp.where(hit, 1.0, 0.0).astype(BF)
        g = weights[r]
        g1 = jnp.minimum(g, BF_MAX).astype(BF).astype(F32)
        rem = g - g1
        g2 = rem.astype(BF).astype(F32)
        g3 = rem - g2
        v = jnp.concatenate([rk, g1, g2, g3], axis=0)
        vt = v.T.astype(BF)
        hit = _dot(vt, pick[0]) == slot_of
        for q in range(3):
            gates[r, q * T:(q + 1) * T, :] = jnp.where(hit, _dot(vt, pick[q + 1]), 0.0).astype(BF)

    def forward(c):
        for mask in (2, 4, 6):
            ag_copy(c, mask).wait_recv()
            fwd_copy(c, mask).start()

    forward(0)
    for kc in range(KC):
        ag_copy(kc, 1).wait_recv()
        for mask in (2, 4, 6):
            fwd_copy(kc, mask).wait_recv()

        width = CHUNKS[kc][1]
        for r in range(N):
            rows = _dot(onehot[r], part(kc, r)[...]).astype(BF)
            for b in range(EL + 1):
                xs[b, r * CAP:(r + 1) * CAP, 0:width] = rows[b * CAP:(b + 1) * CAP]

        def block(b, slot, q, kc=kc, width=width):
            rows = xs[b, :, 0:width]
            for n in range(FF // 256):
                cols = slice(n * 256, (n + 1) * 256)
                a = _dot(rows, ring1[slot, 0, q, 0:width, cols])
                bb = _dot(rows, ring1[slot, 1, q, 0:width, cols])
                if kc > 0:
                    a = a + acc[0, b, :, cols]
                    bb = bb + acc[1, b, :, cols]
                if kc < KC - 1:
                    acc[0, b, :, cols] = a
                    acc[1, b, :, cols] = bb
                else:
                    u[b, :, cols] = (jax.nn.silu(a) * bb).astype(BF)

        def step(p, _, kc=kc):
            i = kc * NP + p
            slot = i % NS
            for c in up_copies(kc, p, slot):
                c.wait()
            for q in range(EP):
                block(p * EP + q, slot, q)

            @pl.when((p == 0) & (me == 0))
            def _():
                block(EL, slot, 0)

            @pl.when(p < NP - NS)
            def _():
                for c in up_copies(kc, p + NS, slot):
                    c.start()

            if kc + 1 < KC:
                @pl.when(p >= NP - NS)
                def _():
                    for c in up_copies(kc + 1, p + NS - NP, slot):
                        c.start()

            if kc + 1 < KC:
                @pl.when(p == FWD_AT)
                def _():
                    forward(kc + 1)
            if kc == KC - 1:
                @pl.when(p < 2)
                def _():
                    down_copy(p).start()
            return 0
        lax.fori_loop(0, NP, step, 0)

    def d_copy(nc):
        return remote(acc.at[nc % 2, pl.ds(4, 4), pl.ds(0, T), pl.ds(0, NW)], r1.at[nc], d_s.at[nc], d_r.at[nc], 1)

    def s1_copies(nc):
        return (remote(r1.at[nc, pl.ds(2, 2), pl.ds(0, 64), :], r2.at[nc, 0], s1_s.at[nc, 0], s1_r.at[nc, 0], 2),
                remote(r1.at[nc, pl.ds(1, 2), pl.ds(64, 64), :], r2.at[nc, 1], s1_s.at[nc, 1], s1_r.at[nc, 1], 4))

    def s2_copies(nc):
        return (remote(r2.at[nc, 0, 0], r3.at[nc, 0], s2_s.at[nc, 0], s2_r.at[nc, 0], 4),
                remote(r2.at[nc, 1, 1], r3.at[nc, 1], s2_s.at[nc, 1], s2_r.at[nc, 1], 2))

    def stage1(nc):
        d_copy(nc).wait_recv()
        for q in range(4):
            r1[nc, q] = r1[nc, q] + acc[nc % 2, q, 0:T, 0:NW]
        for c in s1_copies(nc):
            c.start()

    def stage2(nc):
        ca, cb = s1_copies(nc)
        sa, sb = s2_copies(nc)
        ca.wait_recv()
        r2[nc, 0, 0] = r2[nc, 0, 0] + r1[nc, 1, 0:64]
        sa.start()
        cb.wait_recv()
        r2[nc, 1, 1] = r2[nc, 1, 1] + r1[nc, 3, 64:128]
        sb.start()

    def final(nc):
        for h, c in enumerate(s2_copies(nc)):
            c.wait_recv()
            rows = slice(h * 64, h * 64 + 64)
            val = r1[nc, 0, rows] + r2[nc, h, 1 - h] + r3[nc, h]
            y_ref[rows, pl.ds(pl.multiple_of(nc * NW, NW), NW)] = val.astype(BF)

    def out_step(nc, _):
        down_copy(nc).wait()

        def put(b, e):
            h = _dot(u[b], ring2[nc % 2, e]).astype(BF)
            for r in range(N):
                hbuf[r, b * CAP:(b + 1) * CAP, :] = h[r * CAP:(r + 1) * CAP]
        for e in range(EL):
            put(e, e)

        @pl.when(me == 0)
        def _():
            put(EL, 0)

        @pl.when(nc + 2 < NC)
        def _():
            down_copy(nc + 2).start()

        @pl.when(nc >= 1)
        def _():
            stage1(nc - 1)

        @pl.when(nc >= 2)
        def _():
            d_copy(nc - 2).wait_send()

        def combine(rows):
            for r in (1, 3, 5, 7, 0, 2, 4, 6):
                z = _dot(gates[r, :, 0:rows], hbuf[r, 0:rows, :])
                acc[nc % 2, 4 * (r % 2) + CHIP[r // 2], 0:T, 0:NW] = z[0:T] + z[T:2 * T] + z[2 * T:3 * T]
                if r == 7:
                    d_copy(nc).start()

        @pl.when(me == 0)
        def _():
            combine(RB)

        @pl.when(me != 0)
        def _():
            combine(EL * CAP)

        @pl.when(nc >= 3)
        def _():
            stage2(nc - 3)

        @pl.when(nc >= 5)
        def _():
            final(nc - 5)
        return 0
    lax.fori_loop(0, NC, out_step, 0)
    stage1(NC - 1)
    stage2(NC - 3)
    final(NC - 5)
    stage2(NC - 2)
    final(NC - 4)
    stage2(NC - 1)
    for nc in range(NC - 3, NC):
        final(nc)

    for mask in (1, 2, 4, 6):
        for c in table_copies(mask):
            c.wait_send()
    for mask in (2, 4, 6):
        for c in table_fwd(mask):
            c.wait_send()
    for c in range(KC):
        for mask in (1, 2, 4, 6):
            ag_copy(c, mask).wait_send()
        for mask in (2, 4, 6):
            fwd_copy(c, mask).wait_send()
    for nc in range(NC):
        if nc >= NC - 2:
            d_copy(nc).wait_send()
        for c in s1_copies(nc) + s2_copies(nc):
            c.wait_send()


def _moe(idx, g, x, w1, w3, w2):
    dma = pltpu.SemaphoreType.DMA
    vm, hbm = pl.BlockSpec(memory_space=pltpu.VMEM), pl.BlockSpec(memory_space=pl.ANY)
    return pl.pallas_call(
        _kernel,
        out_shape=jax.ShapeDtypeStruct((T, D), BF),
        in_specs=[vm, vm, vm, hbm, hbm, hbm],
        out_specs=vm,
        scratch_shapes=[
            pltpu.VMEM((N, 8, T), jnp.int32),
            pltpu.VMEM((N, 8, T), F32),
            pltpu.VMEM((2, N, T, 256), BF),
            pltpu.VMEM((3, N, T, 512), BF),
            pltpu.VMEM((N, RB, T), BF),
            pltpu.VMEM((N, 3 * T, RB), BF),
            pltpu.VMEM((EL + 1, N * CAP, KW), BF),
            pltpu.VMEM((2, EL + 1, N * CAP, FF), F32),
            pltpu.VMEM((EL + 1, N * CAP, FF), BF),
            pltpu.VMEM((NS, 2, EP, KW, FF), BF),
            pltpu.VMEM((2, EL, FF, NW), BF),
            pltpu.VMEM((N, RB, NW), BF),
            pltpu.VMEM((NC, 4, T, NW), F32),
            pltpu.VMEM((NC, 2, 2, 64, NW), F32),
            pltpu.VMEM((NC, 2, 64, NW), F32),
            dma((N,)), dma((N,)),
            dma((N,)), dma((N,)),
            dma((KC, N)), dma((KC, N)),
            dma((NS, 2)), dma((2,)),
            dma((NC,)), dma((NC,)),
            dma((NC, 2)), dma((NC, 2)),
            dma((NC, 2)), dma((NC, 2)),
        ],
        compiler_params=pltpu.CompilerParams(collective_id=0, has_side_effects=True, vmem_limit_bytes=67043328),
        name='moe',
    )(idx, g, x, w1, w3, w2)


def solution(mesh):
    def local(x, idx, g, hot_tok, w1, w3, w2):
        return _moe(idx.T, g.T, x, w1, w3, w2)

    rows = P(('data', 'expert'))
    wspec = P('expert')
    return jax.shard_map(local, mesh=mesh, in_specs=(rows, rows, rows, rows, wspec, wspec, wspec), out_specs=rows, check_vma=False)
```

```python
import functools

import jax
import jax.numpy as jnp
from jax import lax
from jax.experimental import pallas as pl
from jax.experimental.pallas import tpu as pltpu
from jax.sharding import PartitionSpec as P

BF = jnp.bfloat16
F32 = jnp.float32
BF_MAX = 3.3895313892515355e38
T = 128
D = 2048
FF = 1024
EL = 8
N = 8
CAP = 32
RB = EL * CAP + CAP
CHUNKS = ((0, 256), (256, 256), (512, 512), (1024, 512), (1536, 512))
KC = len(CHUNKS)
KW = 512
NC = 8
NW = D // NC
EP = 2
NP = EL // EP
NS = 3
FWD_AT = 2
AHEAD = 2
CHIP = (0, 3, 1, 2)


def _dot(a, b):
    return jnp.dot(a, b, preferred_element_type=F32)


def _kernel(idx_hbm, g_hbm, x_hbm, w1_ref, w3_ref, w2_ref, y_hbm,
            idxs, gs, xsmall, xbig, onehot, gates, xs, acc, u, ring1, ring2, hbuf, r1, r2, r3, y_ref, y_sem,
            tab_s, tab_r, gt_s, gt_r, ag_s, ag_r, w1_sem, w2_sem, own_sem, d_s, d_r, s1_s, s1_r, s2_s, s2_r):
    me = lax.axis_index('expert')
    core, xb, yb = me % 2, (me // 2) % 2, me // 4

    def peer(mask):
        return {'expert': me + (mask & 1) * (1 - 2 * core) + ((mask >> 1) & 1) * (2 - 4 * xb) + (mask >> 2) * (4 - 8 * yb)}

    def remote(src, dst, ssem, rsem, mask):
        return pltpu.make_async_remote_copy(src_ref=src, dst_ref=dst, send_sem=ssem, recv_sem=rsem,
                                            device_id=peer(mask), device_id_type=pl.DeviceIdType.MESH)

    def up_copies(kc, p, slot):
        rows = pl.ds(*CHUNKS[kc])
        to = pl.ds(0, CHUNKS[kc][1])
        es = pl.ds(p * EP, EP)
        return (pltpu.make_async_copy(w1_ref.at[es, rows, :], ring1.at[slot, 0, :, to, :], w1_sem.at[slot, 0]),
                pltpu.make_async_copy(w3_ref.at[es, rows, :], ring1.at[slot, 1, :, to, :], w1_sem.at[slot, 1]))

    def down_copy(nc):
        return pltpu.make_async_copy(w2_ref.at[:, :, pl.ds(nc * NW, NW)], ring2.at[nc % 2], w2_sem.at[nc % 2])

    barrier = pltpu.get_barrier_semaphore()
    for mask in range(1, N):
        pl.semaphore_signal(barrier, inc=1, device_id=peer(mask), device_id_type=pl.DeviceIdType.MESH)

    def part(c, mask):
        return xsmall.at[c, mask] if c < 2 else xbig.at[c - 2, mask]

    own = [pltpu.make_async_copy(idx_hbm, idxs.at[0], own_sem.at[KC]),
           pltpu.make_async_copy(g_hbm, gs.at[0], own_sem.at[KC + 1])]
    for c in range(KC):
        own.append(pltpu.make_async_copy(x_hbm.at[:, pl.ds(*CHUNKS[c])], part(c, 0), own_sem.at[c]))
    for c in own:
        c.start()
    for i in range(NS):
        for c in up_copies(0, i, i):
            c.start()

    def table_copies(mask):
        return (remote(idxs.at[0], idxs.at[mask], tab_s.at[mask], tab_r.at[mask], mask),
                remote(gs.at[0], gs.at[mask], gt_s.at[mask], gt_r.at[mask], mask))

    def table_fwd(mask):
        return (remote(idxs.at[mask], idxs.at[mask + 1], tab_s.at[mask + 1], tab_r.at[mask + 1], 1),
                remote(gs.at[mask], gs.at[mask + 1], gt_s.at[mask + 1], gt_r.at[mask + 1], 1))

    def ag_copy(c, mask):
        return remote(part(c, 0), part(c, mask), ag_s.at[c, mask], ag_r.at[c, mask], mask)

    def fwd_copy(c, mask):
        return remote(part(c, mask), part(c, mask + 1), ag_s.at[c, mask + 1], ag_r.at[c, mask + 1], 1)

    for c in own:
        c.wait()
    pl.semaphore_wait(barrier, N - 1)
    for mask in (6, 2, 4, 1):
        for c in table_copies(mask):
            c.start()
    def send(c):
        for mask in (6, 2, 4, 1):
            ag_copy(c, mask).start()

    for c in range(AHEAD):
        send(c)
    for mask in (2, 4, 6):
        for c in table_copies(mask):
            c.wait_recv()
        for c in table_fwd(mask):
            c.start()
    for c in table_copies(1):
        c.wait_recv()
    for mask in (2, 4, 6):
        for c in table_fwd(mask):
            c.wait_recv()

    ids = lax.broadcasted_iota(jnp.int32, (EL, T), 0) + me * EL
    sels, weights = [], []
    for r in range(N):
        sel = jnp.zeros((EL, T), F32)
        gate = jnp.zeros((EL, T), F32)
        tab, gtab = idxs[r], gs[r]
        for j in range(8):
            hit = jnp.broadcast_to(tab[j:j + 1], (EL, T)) == ids
            sel = jnp.where(hit, 1.0, sel)
            gate = jnp.where(hit, jnp.broadcast_to(gtab[j:j + 1], (EL, T)), gate)
        sels.append(sel)
        weights.append(gate)
    sel_all = jnp.concatenate(sels, axis=0)
    upper = (lax.broadcasted_iota(jnp.int32, (T, T), 0) < lax.broadcasted_iota(jnp.int32, (T, T), 1))
    upper = jnp.where(upper, 1.0, 0.0).astype(BF)
    rank_all = jnp.where(sel_all > 0.5, _dot(sel_all.astype(BF), upper), -1.0)

    sub = lax.broadcasted_iota(jnp.int32, (CAP, T), 0).astype(F32)
    for r in range(N):
        for b in range(EL + 1):
            want = sub if b < EL else sub + CAP
            at = r * EL + b % EL
            hit = jnp.broadcast_to(rank_all[at:at + 1], (CAP, T)) == want
            onehot[r, b * CAP:(b + 1) * CAP, :] = jnp.where(hit, 1.0, 0.0).astype(BF)

    def build_gates():
        col = lax.broadcasted_iota(jnp.int32, (32, RB), 1)
        row = lax.broadcasted_iota(jnp.int32, (32, RB), 0)
        owner = jnp.where(col < EL * CAP, col // CAP, 0)
        pick = [jnp.where(row == q * EL + owner, 1.0, 0.0).astype(BF) for q in range(4)]
        colt = lax.broadcasted_iota(jnp.int32, (T, RB), 1)
        slot_of = jnp.where(colt < EL * CAP, colt % CAP, colt - EL * CAP + CAP).astype(F32)
        for r in range(N):
            g = weights[r]
            g1 = jnp.minimum(g, BF_MAX).astype(BF).astype(F32)
            rem = g - g1
            g2 = rem.astype(BF).astype(F32)
            g3 = rem - g2
            v = jnp.concatenate([rank_all[r * EL:(r + 1) * EL], g1, g2, g3], axis=0)
            vt = v.T.astype(BF)
            hit = _dot(vt, pick[0]) == slot_of
            for q in range(3):
                gates[r, q * T:(q + 1) * T, :] = jnp.where(hit, _dot(vt, pick[q + 1]), 0.0).astype(BF)

    def forward(c):
        for mask in (2, 4, 6):
            ag_copy(c, mask).wait_recv()
            fwd_copy(c, mask).start()
        if c + AHEAD < KC:
            send(c + AHEAD)

    forward(0)
    build_gates()
    for kc in range(KC):
        ag_copy(kc, 1).wait_recv()
        for mask in (2, 4, 6):
            fwd_copy(kc, mask).wait_recv()

        width = CHUNKS[kc][1]
        def block(b, slot, q, kc=kc, width=width):
            rows = xs[b, :, 0:width]
            for n in range(FF // 256):
                cols = slice(n * 256, (n + 1) * 256)
                a = _dot(rows, ring1[slot, 0, q, 0:width, cols])
                bb = _dot(rows, ring1[slot, 1, q, 0:width, cols])
                if kc > 0:
                    a = a + acc[0, b, :, cols]
                    bb = bb + acc[1, b, :, cols]
                if kc < KC - 1:
                    acc[0, b, :, cols] = a
                    acc[1, b, :, cols] = bb
                else:
                    u[b, :, cols] = (jax.nn.silu(a) * bb).astype(BF)

        def step(p, _, kc=kc, first=False):
            i = kc * NP + p
            slot = i % NS
            for c in up_copies(kc, p, slot):
                c.wait()
            if first:
                for r in range(N):
                    rows = _dot(onehot[r], part(kc, r)[...]).astype(BF)
                    for b in range(EL + 1):
                        xs[b, r * CAP:(r + 1) * CAP, 0:width] = rows[b * CAP:(b + 1) * CAP]
            for q in range(EP):
                block(p * EP + q, slot, q)

            if first:
                @pl.when(me == 0)
                def _():
                    block(EL, slot, 0)

            @pl.when(p < NP - NS)
            def _():
                for c in up_copies(kc, p + NS, slot):
                    c.start()

            if kc + 1 < KC:
                @pl.when(p >= NP - NS)
                def _():
                    for c in up_copies(kc + 1, p + NS - NP, slot):
                        c.start()

            if kc + 1 < KC:
                @pl.when(p == FWD_AT)
                def _():
                    forward(kc + 1)
            if kc == KC - 1:
                @pl.when(p < 2)
                def _():
                    down_copy(p).start()
            return 0
        step(jnp.int32(0), 0, first=True)
        lax.fori_loop(1, NP, step, 0)

    def d_copy(nc):
        return remote(acc.at[nc % 2, pl.ds(4, 4), pl.ds(0, T), pl.ds(0, NW)], r1.at[nc], d_s.at[nc], d_r.at[nc], 1)

    def s1_copies(nc):
        return (remote(r1.at[nc, pl.ds(2, 2), pl.ds(0, 64), :], r2.at[nc, 0], s1_s.at[nc, 0], s1_r.at[nc, 0], 2),
                remote(r1.at[nc, pl.ds(1, 2), pl.ds(64, 64), :], r2.at[nc, 1], s1_s.at[nc, 1], s1_r.at[nc, 1], 4))

    def s2_copies(nc):
        return (remote(r2.at[nc, 0, 0], r3.at[nc, 0], s2_s.at[nc, 0], s2_r.at[nc, 0], 4),
                remote(r2.at[nc, 1, 1], r3.at[nc, 1], s2_s.at[nc, 1], s2_r.at[nc, 1], 2))

    def stage1(nc):
        d_copy(nc).wait_recv()
        for q in range(4):
            r1[nc, q] = r1[nc, q] + acc[nc % 2, q, 0:T, 0:NW]
        for c in s1_copies(nc):
            c.start()

    def stage2(nc):
        ca, cb = s1_copies(nc)
        sa, sb = s2_copies(nc)
        ca.wait_recv()
        r2[nc, 0, 0] = r2[nc, 0, 0] + r1[nc, 1, 0:64]
        sa.start()
        cb.wait_recv()
        r2[nc, 1, 1] = r2[nc, 1, 1] + r1[nc, 3, 64:128]
        sb.start()

    def y_copy(nc):
        at = pl.ds(pl.multiple_of(nc * NW, NW), NW)
        return pltpu.make_async_copy(y_ref.at[nc], y_hbm.at[:, at], y_sem.at[nc])

    def final(nc):
        for h, c in enumerate(s2_copies(nc)):
            c.wait_recv()
            rows = slice(h * 64, h * 64 + 64)
            val = r1[nc, 0, rows] + r2[nc, h, 1 - h] + r3[nc, h]
            y_ref[nc, rows] = val.astype(BF)
        y_copy(nc).start()

    def out_step(nc, _):

        def put(b, e):
            h = _dot(u[b], ring2[nc % 2, e]).astype(BF)
            for r in range(N):
                hbuf[r, b * CAP:(b + 1) * CAP, :] = h[r * CAP:(r + 1) * CAP]
        for e in range(EL):
            put(e, e)

        @pl.when(me == 0)
        def _():
            put(EL, 0)

        @pl.when(nc + 2 < NC)
        def _():
            down_copy(nc + 2).start()

        @pl.when(nc + 1 < NC)
        def _():
            down_copy(nc + 1).wait()

        @pl.when(nc >= 1)
        def _():
            stage1(nc - 1)

        @pl.when(nc >= 2)
        def _():
            d_copy(nc - 2).wait_send()

        def combine(rows):
            for r in (1, 3, 5, 7, 0, 2, 4, 6):
                z = _dot(gates[r, :, 0:rows], hbuf[r, 0:rows, :])
                acc[nc % 2, 4 * (r % 2) + CHIP[r // 2], 0:T, 0:NW] = z[0:T] + z[T:2 * T] + z[2 * T:3 * T]
                if r == 7:
                    d_copy(nc).start()

        @pl.when(me == 0)
        def _():
            combine(RB)

        @pl.when(me != 0)
        def _():
            combine(EL * CAP)

        @pl.when(nc >= 3)
        def _():
            stage2(nc - 3)

        @pl.when(nc >= 5)
        def _():
            final(nc - 5)
        return 0
    down_copy(0).wait()
    lax.fori_loop(0, NC, out_step, 0)
    stage1(NC - 1)
    stage2(NC - 3)
    final(NC - 5)
    stage2(NC - 2)
    final(NC - 4)
    stage2(NC - 1)
    for nc in range(NC - 3, NC):
        final(nc)

    for mask in (1, 2, 4, 6):
        for c in table_copies(mask):
            c.wait_send()
    for mask in (2, 4, 6):
        for c in table_fwd(mask):
            c.wait_send()
    for c in range(KC):
        for mask in (1, 2, 4, 6):
            ag_copy(c, mask).wait_send()
        for mask in (2, 4, 6):
            fwd_copy(c, mask).wait_send()
    for nc in range(NC):
        if nc >= NC - 2:
            d_copy(nc).wait_send()
        for c in s1_copies(nc) + s2_copies(nc):
            c.wait_send()
        y_copy(nc).wait()


def _moe(idx, g, x, w1, w3, w2):
    dma = pltpu.SemaphoreType.DMA
    hbm = pl.BlockSpec(memory_space=pl.ANY)
    return pl.pallas_call(
        _kernel,
        out_shape=jax.ShapeDtypeStruct((T, D), BF),
        in_specs=[hbm] * 6,
        out_specs=hbm,
        scratch_shapes=[
            pltpu.VMEM((N, 8, T), jnp.int32),
            pltpu.VMEM((N, 8, T), F32),
            pltpu.VMEM((2, N, T, 256), BF),
            pltpu.VMEM((3, N, T, 512), BF),
            pltpu.VMEM((N, RB, T), BF),
            pltpu.VMEM((N, 3 * T, RB), BF),
            pltpu.VMEM((EL + 1, N * CAP, KW), BF),
            pltpu.VMEM((2, EL + 1, N * CAP, FF), F32),
            pltpu.VMEM((EL + 1, N * CAP, FF), BF),
            pltpu.VMEM((NS, 2, EP, KW, FF), BF),
            pltpu.VMEM((2, EL, FF, NW), BF),
            pltpu.VMEM((N, RB, NW), BF),
            pltpu.VMEM((NC, 4, T, NW), F32),
            pltpu.VMEM((NC, 2, 2, 64, NW), F32),
            pltpu.VMEM((NC, 2, 64, NW), F32),
            pltpu.VMEM((NC, T, NW), BF),
            dma((NC,)),
            dma((N,)), dma((N,)),
            dma((N,)), dma((N,)),
            dma((KC, N)), dma((KC, N)),
            dma((NS, 2)), dma((2,)), dma((KC + 2,)),
            dma((NC,)), dma((NC,)),
            dma((NC, 2)), dma((NC, 2)),
            dma((NC, 2)), dma((NC, 2)),
        ],
        compiler_params=pltpu.CompilerParams(collective_id=0, has_side_effects=True, vmem_limit_bytes=67043328),
        name='moe',
    )(idx, g, x, w1, w3, w2)


def solution(mesh):
    def local(x, idx, g, hot_tok, w1, w3, w2):
        return _moe(idx.T, g.T, x, w1, w3, w2)

    rows = P(('data', 'expert'))
    wspec = P('expert')
    return jax.shard_map(local, mesh=mesh, in_specs=(rows, rows, rows, rows, wspec, wspec, wspec), out_specs=rows, check_vma=False)
```

```python
import functools

import jax
import jax.numpy as jnp
from jax import lax
from jax.experimental import pallas as pl
from jax.experimental.pallas import tpu as pltpu
from jax.sharding import PartitionSpec as P

BF = jnp.bfloat16
F32 = jnp.float32
BF_MAX = 3.3895313892515355e38
T = 128
D = 2048
FF = 1024
EL = 8
N = 8
CAP = 32
RB = EL * CAP + CAP
CHUNKS = ((0, 256), (256, 256), (512, 512), (1024, 512), (1536, 512))
KC = len(CHUNKS)
KW = 512
NC = 8
NW = D // NC
EP = 2
NP = EL // EP
NS = 3
FWD_AT = 2
AHEAD = 2
CHIP = (0, 3, 1, 2)


def _dot(a, b):
    return jnp.dot(a, b, preferred_element_type=F32)


def _kernel(idx_hbm, g_hbm, x_hbm, w1_ref, w3_ref, w2_ref, y_hbm,
            idxs, gs, xsmall, xbig, onehot, gates, xs, acc, u, ring1, ring2, r1, r2, r3, y_ref, y_sem,
            tab_s, tab_r, gt_s, gt_r, ag_s, ag_r, w1_sem, w2_sem, own_sem, d_s, d_r, s1_s, s1_r, s2_s, s2_r, l1_s, l1_r, l2_s, l2_r):
    me = lax.axis_index('expert')
    core, xb, yb = me % 2, (me // 2) % 2, me // 4

    def peer(mask):
        return {'expert': me + (mask & 1) * (1 - 2 * core) + ((mask >> 1) & 1) * (2 - 4 * xb) + (mask >> 2) * (4 - 8 * yb)}

    def remote(src, dst, ssem, rsem, mask):
        return pltpu.make_async_remote_copy(src_ref=src, dst_ref=dst, send_sem=ssem, recv_sem=rsem,
                                            device_id=peer(mask), device_id_type=pl.DeviceIdType.MESH)

    def up_copies(kc, p, slot):
        rows = pl.ds(*CHUNKS[kc])
        to = pl.ds(0, CHUNKS[kc][1])
        es = pl.ds(p * EP, EP)
        return (pltpu.make_async_copy(w1_ref.at[es, rows, :], ring1.at[slot, 0, :, to, :], w1_sem.at[slot, 0]),
                pltpu.make_async_copy(w3_ref.at[es, rows, :], ring1.at[slot, 1, :, to, :], w1_sem.at[slot, 1]))

    def down_copy(nc):
        return pltpu.make_async_copy(w2_ref.at[:, :, pl.ds(nc * NW, NW)], ring2.at[nc % 2], w2_sem.at[nc % 2])

    barrier = pltpu.get_barrier_semaphore()
    for mask in (1, 2, 4, 6):
        pl.semaphore_signal(barrier, inc=1, device_id=peer(mask), device_id_type=pl.DeviceIdType.MESH)

    def part(c, mask):
        return xsmall.at[c, mask] if c < 2 else xbig.at[c - 2, mask]

    own = [pltpu.make_async_copy(idx_hbm, idxs.at[0], own_sem.at[KC]),
           pltpu.make_async_copy(g_hbm, gs.at[0], own_sem.at[KC + 1])]
    for c in range(KC):
        own.append(pltpu.make_async_copy(x_hbm.at[:, pl.ds(*CHUNKS[c])], part(c, 0), own_sem.at[c]))
    for c in own:
        c.start()

    def table_copies(mask):
        return (remote(idxs.at[0], idxs.at[mask], tab_s.at[mask], tab_r.at[mask], mask),
                remote(gs.at[0], gs.at[mask], gt_s.at[mask], gt_r.at[mask], mask))

    def table_fwd(mask):
        return (remote(idxs.at[mask], idxs.at[mask + 1], tab_s.at[mask + 1], tab_r.at[mask + 1], 1),
                remote(gs.at[mask], gs.at[mask + 1], gt_s.at[mask + 1], gt_r.at[mask + 1], 1))

    def ag_copy(c, mask):
        return remote(part(c, 0), part(c, mask), ag_s.at[c, mask], ag_r.at[c, mask], mask)

    def fwd_copy(c, mask):
        return remote(part(c, mask), part(c, mask + 1), ag_s.at[c, mask + 1], ag_r.at[c, mask + 1], 1)

    for c in own:
        c.wait()
    pl.semaphore_wait(barrier, 4)
    for mask in (6, 2, 4, 1):
        for c in table_copies(mask):
            c.start()
    def send(c):
        for mask in (6, 2, 4, 1):
            ag_copy(c, mask).start()

    for c in range(AHEAD):
        send(c)
    for i in range(NS):
        for c in up_copies(0, i, i):
            c.start()
    for mask in (2, 4, 6):
        for c in table_copies(mask):
            c.wait_recv()
        for c in table_fwd(mask):
            c.start()
    for c in table_copies(1):
        c.wait_recv()
    for mask in (2, 4, 6):
        for c in table_fwd(mask):
            c.wait_recv()

    ids = lax.broadcasted_iota(jnp.int32, (EL, T), 0) + me * EL
    sels, weights = [], []
    for r in range(N):
        sel = jnp.zeros((EL, T), F32)
        gate = jnp.zeros((EL, T), F32)
        tab, gtab = idxs[r], gs[r]
        for j in range(8):
            hit = jnp.broadcast_to(tab[j:j + 1], (EL, T)) == ids
            sel = jnp.where(hit, 1.0, sel)
            gate = jnp.where(hit, jnp.broadcast_to(gtab[j:j + 1], (EL, T)), gate)
        sels.append(sel)
        weights.append(gate)
    sel_all = jnp.concatenate(sels, axis=0)
    upper = (lax.broadcasted_iota(jnp.int32, (T, T), 0) < lax.broadcasted_iota(jnp.int32, (T, T), 1))
    upper = jnp.where(upper, 1.0, 0.0).astype(BF)
    rank_all = jnp.where(sel_all > 0.5, _dot(sel_all.astype(BF), upper), -1.0)

    sub = lax.broadcasted_iota(jnp.int32, (CAP, T), 0).astype(F32)
    for r in range(N):
        for b in range(EL + 1):
            want = sub if b < EL else sub + CAP
            at = r * EL + b % EL
            hit = jnp.broadcast_to(rank_all[at:at + 1], (CAP, T)) == want
            onehot[r, b * CAP:(b + 1) * CAP, :] = jnp.where(hit, 1.0, 0.0).astype(BF)

    def build_gates():
        col = lax.broadcasted_iota(jnp.int32, (32, RB), 1)
        row = lax.broadcasted_iota(jnp.int32, (32, RB), 0)
        owner = jnp.where(col < EL * CAP, col // CAP, 0)
        pick = [jnp.where(row == q * EL + owner, 1.0, 0.0).astype(BF) for q in range(4)]
        colt = lax.broadcasted_iota(jnp.int32, (T, RB), 1)
        slot_of = jnp.where(colt < EL * CAP, colt % CAP, colt - EL * CAP + CAP).astype(F32)
        for r in range(N):
            g = weights[r]
            g1 = jnp.minimum(g, BF_MAX).astype(BF).astype(F32)
            rem = g - g1
            g2 = rem.astype(BF).astype(F32)
            g3 = rem - g2
            v = jnp.concatenate([rank_all[r * EL:(r + 1) * EL], g1, g2, g3], axis=0)
            vt = v.T.astype(BF)
            hit = _dot(vt, pick[0]) == slot_of
            for q in range(3):
                gates[r, q * T:(q + 1) * T, :] = jnp.where(hit, _dot(vt, pick[q + 1]), 0.0).astype(BF)

    def forward(c):
        for mask in (2, 4, 6):
            ag_copy(c, mask).wait_recv()
            fwd_copy(c, mask).start()
        if c + AHEAD < KC:
            send(c + AHEAD)

    forward(0)
    build_gates()
    for kc in range(KC):
        ag_copy(kc, 1).wait_recv()
        for mask in (2, 4, 6):
            fwd_copy(kc, mask).wait_recv()

        width = CHUNKS[kc][1]
        def block(b, slot, q, kc=kc, width=width):
            rows = xs[b, :, 0:width]
            for n in range(FF // 256):
                cols = slice(n * 256, (n + 1) * 256)
                a = _dot(rows, ring1[slot, 0, q, 0:width, cols])
                bb = _dot(rows, ring1[slot, 1, q, 0:width, cols])
                if kc > 0:
                    a = a + acc[0, b, :, cols]
                    bb = bb + acc[1, b, :, cols]
                if kc < KC - 1:
                    acc[0, b, :, cols] = a
                    acc[1, b, :, cols] = bb
                else:
                    u[b, :, cols] = (jax.nn.silu(a) * bb).astype(BF)

        def step(p, _, kc=kc, first=False):
            i = kc * NP + p
            slot = i % NS
            for c in up_copies(kc, p, slot):
                c.wait()
            if first:
                for r in range(N):
                    rows = _dot(onehot[r], part(kc, r)[...]).astype(BF)
                    for b in range(EL + 1):
                        xs[b, r * CAP:(r + 1) * CAP, 0:width] = rows[b * CAP:(b + 1) * CAP]
            for q in range(EP):
                block(p * EP + q, slot, q)

            if first:
                @pl.when(me == 0)
                def _():
                    block(EL, slot, 0)

            @pl.when(p < NP - NS)
            def _():
                for c in up_copies(kc, p + NS, slot):
                    c.start()

            if kc + 1 < KC:
                @pl.when(p >= NP - NS)
                def _():
                    for c in up_copies(kc + 1, p + NS - NP, slot):
                        c.start()

            if kc + 1 < KC:
                @pl.when(p == FWD_AT)
                def _():
                    forward(kc + 1)
            if kc == KC - 1:
                @pl.when(p < 2)
                def _():
                    down_copy(p).start()
            return 0
        step(jnp.int32(0), 0, first=True)
        lax.fori_loop(1, NP, step, 0)

    def d_copy(nc):
        return remote(acc.at[nc % 2, pl.ds(4, 4), pl.ds(0, T), pl.ds(0, NW)], r1.at[nc], d_s.at[nc], d_r.at[nc], 1)

    def s1_copies(nc):
        return (remote(r1.at[nc, pl.ds(2, 2), pl.ds(0, 64), :], r2.at[nc, 0], s1_s.at[nc, 0], s1_r.at[nc, 0], 2),
                remote(r1.at[nc, pl.ds(1, 2), pl.ds(64, 64), :], r2.at[nc, 1], s1_s.at[nc, 1], s1_r.at[nc, 1], 4))

    def s2_copies(nc):
        return (remote(r2.at[nc, 0, 0], r3.at[nc, 0], s2_s.at[nc, 0], s2_r.at[nc, 0], 4),
                remote(r2.at[nc, 1, 1], r3.at[nc, 1], s2_s.at[nc, 1], s2_r.at[nc, 1], 2))

    LAST = NC - 1

    def last1_copies(h):
        cols = pl.ds(h * 128, 128)
        return (remote(r1.at[LAST, pl.ds(2, 2), pl.ds(0, 64), cols], r2.at[LAST, 0, :, :, cols], l1_s.at[h, 0], l1_r.at[h, 0], 2),
                remote(r1.at[LAST, pl.ds(1, 2), pl.ds(64, 64), cols], r2.at[LAST, 1, :, :, cols], l1_s.at[h, 1], l1_r.at[h, 1], 4))

    def last2_copies(h):
        cols = pl.ds(h * 128, 128)
        return (remote(r2.at[LAST, 0, 0, :, cols], r3.at[LAST, 0, :, cols], l2_s.at[h, 0], l2_r.at[h, 0], 4),
                remote(r2.at[LAST, 1, 1, :, cols], r3.at[LAST, 1, :, cols], l2_s.at[h, 1], l2_r.at[h, 1], 2))

    def last1(h):
        cols = slice(h * 128, h * 128 + 128)
        for q in (2, 3, 1, 0):
            r1[LAST, q, :, cols] = r1[LAST, q, :, cols] + acc[LAST % 2, q, 0:T, cols]
        for c in last1_copies(h):
            c.start()

    def last2(h):
        cols = slice(h * 128, h * 128 + 128)
        ca, cb = last1_copies(h)
        sa, sb = last2_copies(h)
        ca.wait_recv()
        r2[LAST, 0, 0, :, cols] = r2[LAST, 0, 0, :, cols] + r1[LAST, 1, 0:64, cols]
        sa.start()
        cb.wait_recv()
        r2[LAST, 1, 1, :, cols] = r2[LAST, 1, 1, :, cols] + r1[LAST, 3, 64:128, cols]
        sb.start()

    def last_final():
        for h in range(2):
            cols = slice(h * 128, h * 128 + 128)
            for k, c in enumerate(last2_copies(h)):
                c.wait_recv()
                rows = slice(k * 64, k * 64 + 64)
                val = r1[LAST, 0, rows, cols] + r2[LAST, k, 1 - k, :, cols] + r3[LAST, k, :, cols]
                y_ref[LAST, rows, cols] = val.astype(BF)
        y_copy(LAST).start()

    def stage1(nc):
        d_copy(nc).wait_recv()
        for q in range(4):
            r1[nc, q] = r1[nc, q] + acc[nc % 2, q, 0:T, 0:NW]
        for c in s1_copies(nc):
            c.start()

    def stage2(nc):
        ca, cb = s1_copies(nc)
        sa, sb = s2_copies(nc)
        ca.wait_recv()
        r2[nc, 0, 0] = r2[nc, 0, 0] + r1[nc, 1, 0:64]
        sa.start()
        cb.wait_recv()
        r2[nc, 1, 1] = r2[nc, 1, 1] + r1[nc, 3, 64:128]
        sb.start()

    def y_copy(nc):
        at = pl.ds(pl.multiple_of(nc * NW, NW), NW)
        return pltpu.make_async_copy(y_ref.at[nc], y_hbm.at[:, at], y_sem.at[nc])

    def final(nc):
        for h, c in enumerate(s2_copies(nc)):
            c.wait_recv()
            rows = slice(h * 64, h * 64 + 64)
            val = r1[nc, 0, rows] + r2[nc, h, 1 - h] + r3[nc, h]
            y_ref[nc, rows] = val.astype(BF)
        y_copy(nc).start()

    def out_step(nc, _):

        def put(b, e):
            h = _dot(u[b], ring2[nc % 2, e]).astype(BF)
            for r in range(N):
                if b < EL:
                    xs[r, b * CAP:(b + 1) * CAP, 0:NW] = h[r * CAP:(r + 1) * CAP]
                else:
                    xs[r, 0:CAP, NW:2 * NW] = h[r * CAP:(r + 1) * CAP]
        for e in range(EL):
            put(e, e)

        @pl.when(me == 0)
        def _():
            put(EL, 0)

        @pl.when(nc + 2 < NC)
        def _():
            down_copy(nc + 2).start()

        @pl.when(nc + 1 < NC)
        def _():
            down_copy(nc + 1).wait()

        @pl.when(nc >= 1)
        def _():
            stage1(nc - 1)

        @pl.when(nc >= 2)
        def _():
            d_copy(nc - 2).wait_send()

        def combine(second):
            for r in (1, 3, 5, 7, 0, 2, 4, 6):
                z = _dot(gates[r, :, 0:EL * CAP], xs[r, :, 0:NW])
                if second:
                    z = z + _dot(gates[r, :, EL * CAP:RB], xs[r, 0:CAP, NW:2 * NW])
                acc[nc % 2, 4 * (r % 2) + CHIP[r // 2], 0:T, 0:NW] = z[0:T] + z[T:2 * T] + z[2 * T:3 * T]
                if r == 7:
                    d_copy(nc).start()

        @pl.when(me == 0)
        def _():
            combine(True)

        @pl.when(me != 0)
        def _():
            combine(False)

        @pl.when(nc >= 3)
        def _():
            stage2(nc - 3)

        @pl.when(nc >= 5)
        def _():
            final(nc - 5)
        return 0
    down_copy(0).wait()
    lax.fori_loop(0, NC, out_step, 0)
    d_copy(LAST).wait_recv()
    last1(0)
    last1(1)
    stage2(NC - 3)
    final(NC - 5)
    stage2(NC - 2)
    final(NC - 4)
    last2(0)
    last2(1)
    final(NC - 3)
    final(NC - 2)
    last_final()

    for mask in (1, 2, 4, 6):
        for c in table_copies(mask):
            c.wait_send()
    for mask in (2, 4, 6):
        for c in table_fwd(mask):
            c.wait_send()
    for c in range(KC):
        for mask in (1, 2, 4, 6):
            ag_copy(c, mask).wait_send()
        for mask in (2, 4, 6):
            fwd_copy(c, mask).wait_send()
    for nc in range(NC):
        if nc >= NC - 2:
            d_copy(nc).wait_send()
        if nc < LAST:
            for c in s1_copies(nc) + s2_copies(nc):
                c.wait_send()
        y_copy(nc).wait()
    for h in range(2):
        for c in last1_copies(h) + last2_copies(h):
            c.wait_send()


def _moe(idx, g, x, w1, w3, w2):
    dma = pltpu.SemaphoreType.DMA
    hbm = pl.BlockSpec(memory_space=pl.ANY)
    return pl.pallas_call(
        _kernel,
        out_shape=jax.ShapeDtypeStruct((T, D), BF),
        in_specs=[hbm] * 6,
        out_specs=hbm,
        scratch_shapes=[
            pltpu.VMEM((N, 8, T), jnp.int32),
            pltpu.VMEM((N, 8, T), F32),
            pltpu.VMEM((2, N, T, 256), BF),
            pltpu.VMEM((3, N, T, 512), BF),
            pltpu.VMEM((N, RB, T), BF),
            pltpu.VMEM((N, 3 * T, RB), BF),
            pltpu.VMEM((EL + 1, N * CAP, KW), BF),
            pltpu.VMEM((2, EL + 1, N * CAP, FF), F32),
            pltpu.VMEM((EL + 1, N * CAP, FF), BF),
            pltpu.VMEM((NS, 2, EP, KW, FF), BF),
            pltpu.VMEM((2, EL, FF, NW), BF),
            pltpu.VMEM((NC, 4, T, NW), F32),
            pltpu.VMEM((NC, 2, 2, 64, NW), F32),
            pltpu.VMEM((NC, 2, 64, NW), F32),
            pltpu.VMEM((NC, T, NW), BF),
            dma((NC,)),
            dma((N,)), dma((N,)),
            dma((N,)), dma((N,)),
            dma((KC, N)), dma((KC, N)),
            dma((NS, 2)), dma((2,)), dma((KC + 2,)),
            dma((NC,)), dma((NC,)),
            dma((NC, 2)), dma((NC, 2)),
            dma((NC, 2)), dma((NC, 2)),
            dma((2, 2)), dma((2, 2)),
            dma((2, 2)), dma((2, 2)),
        ],
        compiler_params=pltpu.CompilerParams(collective_id=0, has_side_effects=True, vmem_limit_bytes=67043328),
        name='moe',
    )(idx, g, x, w1, w3, w2)


def solution(mesh):
    def local(x, idx, g, hot_tok, w1, w3, w2):
        return _moe(idx.T, g.T, x, w1, w3, w2)

    rows = P(('data', 'expert'))
    wspec = P('expert')
    return jax.shard_map(local, mesh=mesh, in_specs=(rows, rows, rows, rows, wspec, wspec, wspec), out_specs=rows, check_vma=False)
```
